32 devices in a mesh: batch: 4 (over z), seq: 8 (over y, x, core).
Axes of the slice: x: 2, y: 2, z: 4, core: 2. Of those that a mesh axis runs over, the one named last changes fastest.
Arguments:
- tokens: bfloat16 [10240, 8192], P(('batch', 'seq')), may hold values from -6 to 6
- out_grad: bfloat16 [10240, 8192], P(('batch', 'seq')), may hold values from -0.109375 to 0.109375
- gate_pre: bfloat16 [10240, 768], P(('batch', 'seq')), may hold values from -8 to 8
- up_pre: bfloat16 [10240, 768], P(('batch', 'seq')), may hold values from -6 to 6
- hidden_grad: bfloat16 [10240, 768], P(('batch', 'seq')), may hold values from -0.0625 to 0.0625
Outputs:
- gate_weight_grad: float32 [8192, 768], P(('seq', 'batch'))
- up_weight_grad: float32 [8192, 768], P(('seq', 'batch'))
- down_weight_grad: float32 [8192, 768], P(('seq', 'batch'))
The draws below stay inside these ranges and needn't reach their ends.
All inputs are finite; a program needn't handle non-finite values.
Results may differ from the reference program's by a relative error of at most 0.019.
Values may be sent and summed in bfloat16 or wider, within the bound.
A program may use at most 192 MiB of HBM per device.

```python
import jax
import jax.numpy as jnp
from jax import lax

D = 8192
FF = 768
TOK_DEV = 320
TOKENS = 10240
N_BATCH = 4
N_SEQ = 8


def strengthened(result, stream_key, source, target, blocks, factor):
    owner, partner = [(jnp.arange(result.shape[position]) // (result.shape[position] // blocks)).reshape([-1 if axis == position else 1 for axis in range(result.ndim)]) for position in (source, target)]
    chosen = jax.random.permutation(stream_key, blocks)[partner]
    strong = (owner == chosen) | (owner == (partner + blocks // 2) % blocks)
    return jnp.where(strong, factor * result, result)


def shard_levels(rng, shape, cuts, smallest, top_value):
    factor_of, own = 1.0, jax.random.fold_in(rng, 6)
    for position, blocks in cuts:
        steps = jnp.exp(jax.random.uniform(jax.random.fold_in(own, position), (blocks,), jnp.float32, smallest / len(cuts), top_value / len(cuts)))
        factor_of = factor_of * jnp.repeat(steps, shape[position] // blocks).reshape([-1 if axis == position else 1 for axis in range(len(shape))])
    return factor_of


def gaussian(own_key, extent, deviation, reach, split=(), kind=jnp.bfloat16):
    array = deviation * jax.random.normal(own_key, extent, jnp.float32)
    if split:
        array = array * shard_levels(own_key, extent, split, -0.22, 0.18)
    return jnp.clip(array, -reach, reach).astype(kind)


def heavy_noise(own_key, extent, width, most, split, heavy, kind=jnp.bfloat16):
    entries = width * jax.random.normal(own_key, extent, jnp.float32)
    if split:
        entries = entries * shard_levels(own_key, extent, split, -0.22, 0.18)
    return jnp.clip(strengthened(entries, jax.random.fold_in(own_key, 3), *heavy), -most, most).astype(kind)


def setup_inputs(seed: int = 0) -> dict:
    key_of = jax.random.split(jax.random.key(seed), 6)
    tokens = heavy_noise(key_of[0], (TOKENS, D), 1.0, 6.0, ((0, 32),), (0, 1, 32, 2.75))
    out_grad = heavy_noise(key_of[1], (TOKENS, D), TOKENS ** -0.5, 0.109375, ((0, 32),), (0, 1, 32, 2.75))
    gate_pre = gaussian(key_of[2], (TOKENS, FF), 1.5, 8.0, ((0, 32),))
    up_pre = gaussian(key_of[3], (TOKENS, FF), 1.0, 6.0, ((0, 32),))
    hidden_grad = gaussian(key_of[4], (TOKENS, FF), TOKENS ** -0.5, 0.0625, ((0, 32),))
    return {"tokens": tokens, "out_grad": out_grad, "gate_pre": gate_pre, "up_pre": up_pre, "hidden_grad": hidden_grad}


def hidden_parts(gate_pre, up_pre, hidden_grad):
    gate_val = gate_pre.astype(jnp.float32)
    up_val = up_pre.astype(jnp.float32)
    grad_val = hidden_grad.astype(jnp.float32)
    sigmoid_val = jax.nn.sigmoid(gate_val)
    activated = gate_val * sigmoid_val
    hidden = (activated * up_val).astype(jnp.bfloat16)
    up_cotangent = (grad_val * activated).astype(jnp.bfloat16)
    gate_cotangent = (grad_val * up_val * sigmoid_val * (1.0 + gate_val * (1.0 - sigmoid_val))).astype(jnp.bfloat16)
    return hidden, gate_cotangent, up_cotangent


def contract_rows(left, right):
    return lax.dot_general(left, right, (((0,), (0,)), ((), ())), preferred_element_type=jnp.float32)


def reference(tokens, out_grad, gate_pre, up_pre, hidden_grad):
    hidden, gate_cotangent, up_cotangent = hidden_parts(gate_pre, up_pre, hidden_grad)
    cotangents = jnp.concatenate([gate_cotangent, up_cotangent], axis=1)
    blocks = N_BATCH * N_SEQ
    model_width = tokens.shape[1]
    hidden_width = hidden.shape[1]

    def add_block(total, pieces):
        features, grads, cotangent_rows, hidden_slice = pieces
        term = jnp.concatenate([contract_rows(features, cotangent_rows), contract_rows(grads, hidden_slice)], axis=1)
        return total + lax.optimization_barrier(term.astype(jnp.bfloat16)).astype(jnp.float32), None

    pieces = (tokens.reshape(blocks, TOK_DEV, model_width), out_grad.reshape(blocks, TOK_DEV, model_width),
              cotangents.reshape(blocks, TOK_DEV, 2 * hidden_width), hidden.reshape(blocks, TOK_DEV, hidden_width))
    total, unused = lax.scan(add_block, jnp.zeros((model_width, 3 * hidden_width), jnp.float32), pieces)
    return (total[:, :hidden_width], total[:, hidden_width:2 * hidden_width], total[:, 2 * hidden_width:])
```

```python
import functools

import jax
import jax.numpy as jnp
from jax import lax
from jax.experimental import pallas as pl
from jax.experimental.pallas import tpu as pltpu
from jax.sharding import PartitionSpec as P

MESH = pl.DeviceIdType.MESH
LANES = 128


def bit_count(n):
    return n.bit_length() - 1


def flip(value, mask):
    if isinstance(mask, int) and mask == 0:
        return value
    out, bit = 0, 1
    top = mask if isinstance(mask, int) else 1 << 10
    out = value
    while bit <= top:
        if isinstance(mask, int):
            if mask & bit:
                out = out + bit * (1 - 2 * ((value // bit) % 2))
        else:
            out = out + ((mask // bit) % 2) * bit * (1 - 2 * ((value // bit) % 2))
        bit *= 2
    return out


def flip_traced(value, mask, bits):
    out = value
    for i in range(bits):
        bit = 1 << i
        out = out + ((mask // bit) % 2) * bit * (1 - 2 * ((value // bit) % 2))
    return out


class Plan:
    def __init__(self, n_batch, n_seq, tok, width, hidden):
        self.n_batch, self.n_seq, self.tok, self.width, self.hidden = n_batch, n_seq, tok, width, hidden
        self.chips = n_seq // 2
        self.seq_bits, self.batch_bits = bit_count(self.chips), bit_count(n_batch)
        self.rows = width // (n_batch * n_seq)
        self.group = max(1, LANES // self.rows)
        self.block = self.group * self.rows
        self.n_groups = n_batch // self.group
        total = 3 * hidden
        units = total // LANES
        late = max(1, units // 9)
        early = (units - 2 * late) // 2
        cuts = [0, early, units - 2 * late, units - late, units]
        self.spans = [(a * LANES, b * LANES) for a, b in zip(cuts[:-1], cuts[1:])]
        self.ascending = [True, False, True, False]
        self.batch_first = [False, False, True, True]

    def seq_bit(self, cls, stage):
        return stage if self.ascending[cls] else self.seq_bits - 1 - stage

    def position(self, cls, u):
        if not self.ascending[cls]:
            return u
        return sum(((u // (1 << i)) % 2) * (1 << (self.seq_bits - 1 - i)) for i in range(self.seq_bits))

    def pieces(self, lo, hi, step):
        out = []
        while lo < hi:
            end = min(hi, (lo // step + 1) * step)
            out.append((lo, end))
            lo = end
        return out


def low_bit(m):
    return (m & -m).bit_length() - 1


def kernel(plan, tokens, out_grad, gate_pre, up_pre, hidden_grad, out_gate, out_up, out_down, *scratch):
    p = plan
    T, R, M, C, NB = p.tok, p.rows, p.block, p.chips, p.n_batch
    n_cls, sb, bb = len(p.spans), p.seq_bits, p.batch_bits
    scratch = list(scratch)
    raw, hid, tok_v, grad_v = (scratch.pop(0) for _ in range(4))
    terms = [scratch.pop(0) for _ in range(n_cls)]
    seq_in = [[scratch.pop(0) for _ in range(sb)] for _ in range(n_cls)]
    batch_in = [[scratch.pop(0) for _ in range(bb)] for _ in range(n_cls)]
    raw_sem, load_sem, swap_sem, swap_out, seq_send, seq_recv, batch_send, batch_recv = scratch
    outs = (out_gate, out_up, out_down)

    b_me, s_me = lax.axis_index("batch"), lax.axis_index("seq")
    core, chip = s_me % 2, s_me // 2
    twin = (b_me, s_me + 1 - 2 * core)
    seq_peer = [(b_me, flip(s_me, 2 << i)) for i in range(sb)]
    batch_peer = [(flip(b_me, 1 << i), s_me) for i in range(bb)]

    pre = (gate_pre, up_pre, hidden_grad)
    for i, ref in enumerate(pre):
        pltpu.make_async_copy(ref, raw.at[0, i], raw_sem.at[0]).start()

    def column(g, u, side):
        k = flip(chip, u)
        first = flip(b_me // p.group, g) * p.group
        return pl.multiple_of(((k * 2 + side) * NB + first) * R, M)

    sends = []
    groups = list(range(p.n_groups - 1, -1, -1))

    def load(g):
        for a, (src, dst) in enumerate(((tokens, tok_v), (out_grad, grad_v))):
            for u in range(C):
                pltpu.make_async_copy(
                    src.at[:, pl.ds(column(g, u, core), M)], dst.at[g, 0, u], load_sem.at[g, a]
                ).start()

    def swap(g):
        for a, (src, dst) in enumerate(((tokens, tok_v), (out_grad, grad_v))):
            for u in range(C):
                pltpu.make_async_remote_copy(
                    src_ref=src.at[:, pl.ds(column(g, u, 1 - core), M)],
                    dst_ref=dst.at[g, 1, u],
                    send_sem=swap_out.at[g, a],
                    recv_sem=swap_sem.at[g, a],
                    device_id=twin,
                    device_id_type=MESH,
                ).start()

    for g in groups:
        load(g)

    barrier = pltpu.get_barrier_semaphore()
    peers = [twin] + seq_peer + batch_peer
    for peer in peers:
        pl.semaphore_signal(barrier, inc=1, device_id=peer, device_id_type=MESH)
    pl.semaphore_wait(barrier, len(peers))

    for i, ref in enumerate(pre):
        pltpu.make_async_remote_copy(
            src_ref=ref, dst_ref=raw.at[1, i], send_sem=raw_sem.at[1], recv_sem=raw_sem.at[2],
            device_id=twin, device_id_type=MESH,
        ).start()
    for g in groups:
        swap(g)

    def activate(side):
        step = 32
        def body(i, carry):
            at = pl.ds(pl.multiple_of(i * step, step), step)
            gate_val = raw[side, 0, at, :].astype(jnp.float32)
            up_val = raw[side, 1, at, :].astype(jnp.float32)
            grad_val = raw[side, 2, at, :].astype(jnp.float32)
            sig = jax.nn.sigmoid(gate_val)
            act = gate_val * sig
            F = p.hidden
            hid[side, at, 0:F] = (grad_val * up_val * sig * (1.0 + gate_val * (1.0 - sig))).astype(jnp.bfloat16)
            hid[side, at, F:2 * F] = (grad_val * act).astype(jnp.bfloat16)
            hid[side, at, 2 * F:3 * F] = (act * up_val).astype(jnp.bfloat16)
            return carry
        lax.fori_loop(0, T // step, body, 0)

    def wait_bytes(ref, sem):
        pltpu.make_async_copy(ref, ref, sem).wait()

    wait_bytes(raw.at[0], raw_sem.at[0])
    activate(0)
    wait_bytes(raw.at[1], raw_sem.at[2])
    activate(1)

    def dots(lhs, lo, hi):
        total = None
        for side in range(2):
            part = lax.dot_general(
                lhs[side], hid[side, :, lo:hi], (((0,), (0,)), ((), ())), preferred_element_type=jnp.float32
            )
            total = part if total is None else total + part
        return total

    def compute(g):
        for a, dst in enumerate((tok_v, grad_v)):
            wait_bytes(dst.at[g, 0], load_sem.at[g, a])
            wait_bytes(dst.at[g, 1], swap_sem.at[g, a])

        def body(u, carry):
            feats = [tok_v[g, side, u] for side in range(2)]
            grads = [grad_v[g, side, u] for side in range(2)]
            for cls, (lo, hi) in enumerate(p.spans):
                pos = p.position(cls, u)
                for a, b in p.pieces(lo, hi, 2 * p.hidden):
                    value = dots(feats if a < 2 * p.hidden else grads, a, b).astype(jnp.bfloat16)
                    for h in range(p.group):
                        m = g if p.group == 1 else g * p.group + flip(b_me % p.group, h)
                        terms[cls][m, pos, :, a - lo:b - lo] = value[h * R:(h + 1) * R]
            return carry
        lax.fori_loop(0, C, body, 0)

    step = min(R, 32)

    def gather(cls, m, first, count, extra):
        def body(i, carry):
            blk, at = first + i // (R // step), pl.ds(pl.multiple_of((i % (R // step)) * step, step), step)
            value = terms[cls][m, blk, at, :].astype(jnp.float32)
            for ref, slot in extra:
                value = value + ref[slot, blk, at, :].astype(jnp.float32)
            terms[cls][m, blk, at, :] = value.astype(jnp.bfloat16)
            return carry
        if extra:
            lax.fori_loop(0, count * (R // step), body, 0)

    def finish(cls, extra):
        lo, hi = p.spans[cls]
        def body(i, carry):
            at = pl.ds(pl.multiple_of(i * step, step), step)
            for a, b in p.pieces(lo, hi, p.hidden):
                value = terms[cls][0, 0, at, a - lo:b - lo].astype(jnp.float32)
                for ref, slot in extra:
                    value = value + ref[slot, 0, at, a - lo:b - lo].astype(jnp.float32)
                base = (a // p.hidden) * p.hidden
                outs[a // p.hidden][at, a - base:b - base] = value
            return carry
        lax.fori_loop(0, R // step, body, 0)

    def seq_slot(cls, m):
        return 0 if p.batch_first[cls] else m

    def seq_copy(cls, m, stage):
        count = C >> (stage + 1)
        slot = seq_slot(cls, m)
        return pltpu.make_async_remote_copy(
            src_ref=terms[cls].at[m, pl.ds(count, count)],
            dst_ref=seq_in[cls][stage].at[slot],
            send_sem=seq_send.at[cls, stage, slot],
            recv_sem=seq_recv.at[cls, stage, slot],
            device_id=seq_peer[p.seq_bit(cls, stage)],
            device_id_type=MESH,
        )

    def batch_copy(cls, m):
        stage = low_bit(m)
        slot = m >> (stage + 1)
        count = C if p.batch_first[cls] else 1
        return pltpu.make_async_remote_copy(
            src_ref=terms[cls].at[m, pl.ds(0, count)],
            dst_ref=batch_in[cls][stage].at[slot],
            send_sem=batch_send.at[cls, stage, slot],
            recv_sem=batch_recv.at[cls, stage, slot],
            device_id=batch_peer[stage],
            device_id_type=MESH,
        )

    def start(copy):
        copy.start()
        sends.append(copy)

    def from_seq(cls, m, stages):
        return [(seq_in[cls][j], seq_slot(cls, m)) for j in range(stages)]

    def from_batch(cls, m):
        count = bb if m == 0 else low_bit(m)
        return [(batch_in[cls][j], m >> (j + 1)) for j in range(count)]

    def wait_batch(cls, m):
        count = bb if m == 0 else low_bit(m)
        for j in range(count):
            batch_copy(cls, m + (1 << j)).wait_recv()

    def seq_stage(cls, m, stage, base):
        if stage:
            seq_copy(cls, m, stage - 1).wait_recv()
        count = C >> (stage + 1)
        gather(cls, m, count, count, base + from_seq(cls, m, stage))
        start(seq_copy(cls, m, stage))

    def batch_last(cls, m):
        seq_copy(cls, m, sb - 1).wait_recv()
        wait_batch(cls, m)
        extra = from_seq(cls, m, sb) + from_batch(cls, m)
        if m == 0:
            finish(cls, extra)
        else:
            gather(cls, m, 0, 1, extra)
            start(batch_copy(cls, m))

    def batch_early(cls, m):
        wait_batch(cls, m)
        if m:
            gather(cls, m, 0, C, from_batch(cls, m))
            start(batch_copy(cls, m))
        else:
            seq_stage(cls, 0, 0, from_batch(cls, 0))

    plain = [c for c in range(n_cls) if not p.batch_first[c]]
    early = [c for c in range(n_cls) if p.batch_first[c]]
    order = list(range(NB - 1, -1, -1))
    done = set()
    for i in range(NB + 2):
        if i < NB:
            m = order[i]
            if m // p.group not in done:
                done.add(m // p.group)
                compute(m // p.group)
            for cls in plain:
                seq_stage(cls, m, 0, [])
            if m % 2:
                for cls in early:
                    batch_early(cls, m)
        if 1 <= i <= NB:
            m = order[i - 1]
            if m == 0:
                for cls in early:
                    batch_early(cls, m)
            for stage in range(1, sb):
                for cls in plain:
                    seq_stage(cls, m, stage, [])
            if m and m % 2 == 0:
                for cls in early:
                    batch_early(cls, m)
        if i == NB + 1:
            for stage in range(1, sb):
                for cls in early:
                    seq_stage(cls, 0, stage, from_batch(cls, 0))
        if i >= 2:
            for cls in plain:
                batch_last(cls, order[i - 2])
    for cls in early:
        seq_copy(cls, 0, sb - 1).wait_recv()
        finish(cls, from_batch(cls, 0) + from_seq(cls, 0, sb))

    for copy in sends:
        copy.wait_send()
    wait_bytes(raw.at[1], raw_sem.at[1])
    for g in groups:
        for a, dst in enumerate((tok_v, grad_v)):
            wait_bytes(dst.at[g, 1], swap_out.at[g, a])


def on_device(n_batch, n_seq, tokens, out_grad, gate_pre, up_pre, hidden_grad):
    tok, width = tokens.shape
    hidden = gate_pre.shape[1]
    p = Plan(n_batch, n_seq, tok, width, hidden)
    C, R, bf16 = p.chips, p.rows, jnp.bfloat16
    scratch = [
        pltpu.VMEM((2, 3, tok, hidden), bf16),
        pltpu.VMEM((2, tok, 3 * hidden), bf16),
        pltpu.VMEM((p.n_groups, 2, C, tok, p.block), bf16),
        pltpu.VMEM((p.n_groups, 2, C, tok, p.block), bf16),
    ]
    sizes = [hi - lo for lo, hi in p.spans]
    scratch += [pltpu.VMEM((n_batch, C, R, size), bf16) for size in sizes]
    for cls, size in enumerate(sizes):
        slots = 1 if p.batch_first[cls] else n_batch
        scratch += [pltpu.VMEM((slots, C >> (j + 1), R, size), bf16) for j in range(p.seq_bits)]
    for cls, size in enumerate(sizes):
        blocks = C if p.batch_first[cls] else 1
        scratch += [pltpu.VMEM((n_batch >> (j + 1), blocks, R, size), bf16) for j in range(p.batch_bits)]
    n_cls = len(sizes)
    dma = pltpu.SemaphoreType.DMA
    scratch += [
        dma((3,)),
        dma((p.n_groups, 2)), dma((p.n_groups, 2)), dma((p.n_groups, 2)),
        dma((n_cls, p.seq_bits, n_batch)), dma((n_cls, p.seq_bits, n_batch)),
        dma((n_cls, p.batch_bits, n_batch // 2)), dma((n_cls, p.batch_bits, n_batch // 2)),
    ]
    out = jax.ShapeDtypeStruct((R, hidden), jnp.float32)
    return pl.pallas_call(
        functools.partial(kernel, p),
        out_shape=(out, out, out),
        in_specs=[pl.BlockSpec(memory_space=pltpu.HBM)] * 5,
        out_specs=[pl.BlockSpec(memory_space=pltpu.VMEM)] * 3,
        scratch_shapes=scratch,
        compiler_params=pltpu.CompilerParams(
            collective_id=0, has_side_effects=True, vmem_limit_bytes=67043328
        ),
    )(tokens, out_grad, gate_pre, up_pre, hidden_grad)


def solution(mesh):
    rows = P(("batch", "seq"), None)
    outs = P(("seq", "batch"), None)
    body = functools.partial(on_device, mesh.shape["batch"], mesh.shape["seq"])
    return jax.shard_map(
        body, mesh=mesh, in_specs=(rows,) * 5, out_specs=(outs,) * 3, check_vma=False
    )
```

```python
import functools

import jax
import jax.numpy as jnp
from jax import lax
from jax.experimental import pallas as pl
from jax.experimental.pallas import tpu as pltpu
from jax.sharding import PartitionSpec as P

MESH = pl.DeviceIdType.MESH
LANES = 128


def bit_count(n):
    return n.bit_length() - 1


def flip(value, mask):
    out, bit = value, 1
    while bit <= mask:
        if mask & bit:
            out = out + bit * (1 - 2 * ((value // bit) % 2))
        bit *= 2
    return out


class Plan:
    def __init__(self, n_batch, n_seq, tok, width, hidden):
        self.n_batch, self.n_seq, self.tok, self.width, self.hidden = n_batch, n_seq, tok, width, hidden
        self.chips = n_seq // 2
        self.seq_bits, self.batch_bits = bit_count(self.chips), bit_count(n_batch)
        self.rows = width // (n_batch * n_seq)
        self.group = max(1, LANES // self.rows)
        self.block = self.group * self.rows
        self.n_groups = n_batch // self.group
        total = 3 * hidden
        units = total // LANES
        late = max(1, units // 9)
        early = (units - 2 * late) // 2
        cuts = [0, early, units - 2 * late, units - late, units]
        self.spans = [(a * LANES, b * LANES) for a, b in zip(cuts[:-1], cuts[1:])]
        self.ascending = [True, False, True, False]
        self.batch_first = [False, False, True, True]

    def seq_bit(self, cls, stage):
        return stage if self.ascending[cls] else self.seq_bits - 1 - stage

    def position(self, cls, u):
        if not self.ascending[cls]:
            return u
        return sum(((u // (1 << i)) % 2) * (1 << (self.seq_bits - 1 - i)) for i in range(self.seq_bits))

    def pieces(self, lo, hi, step):
        out = []
        while lo < hi:
            end = min(hi, (lo // step + 1) * step)
            out.append((lo, end))
            lo = end
        return out


def low_bit(m):
    return (m & -m).bit_length() - 1


def kernel(plan, tokens, out_grad, gate_pre, up_pre, hidden_grad, out_gate, out_up, out_down, *scratch):
    p = plan
    T, R, M, C, NB = p.tok, p.rows, p.block, p.chips, p.n_batch
    n_cls, sb, bb = len(p.spans), p.seq_bits, p.batch_bits
    scratch = list(scratch)
    raw, hid, tok_v, grad_v = (scratch.pop(0) for _ in range(4))
    terms = [scratch.pop(0) for _ in range(n_cls)]
    seq_in = [[scratch.pop(0) for _ in range(sb)] for _ in range(n_cls)]
    batch_in = [[scratch.pop(0) for _ in range(bb)] for _ in range(n_cls)]
    raw_sem, load_sem, swap_sem, swap_out, seq_send, seq_recv, batch_send, batch_recv = scratch
    outs = (out_gate, out_up, out_down)

    b_me, s_me = lax.axis_index("batch"), lax.axis_index("seq")
    core, chip = s_me % 2, s_me // 2
    twin = (b_me, s_me + 1 - 2 * core)
    seq_peer = [(b_me, flip(s_me, 2 << i)) for i in range(sb)]
    batch_peer = [(flip(b_me, 1 << i), s_me) for i in range(bb)]

    pre = (gate_pre, up_pre, hidden_grad)
    for i, ref in enumerate(pre):
        pltpu.make_async_copy(ref, raw.at[i, pl.ds(0, T)], raw_sem.at[0]).start()

    def column(g, u, side):
        k = flip(chip, u)
        first = flip(b_me // p.group, g) * p.group
        return pl.multiple_of(((k * 2 + side) * NB + first) * R, M)

    sends = []
    groups = list(range(p.n_groups - 1, -1, -1))

    def load(g):
        for a, (src, dst) in enumerate(((tokens, tok_v), (out_grad, grad_v))):
            for u in range(C):
                pltpu.make_async_copy(
                    src.at[:, pl.ds(column(g, u, core), M)], dst.at[g, u, pl.ds(0, T)], load_sem.at[g, a]
                ).start()

    def swap(g):
        for a, (src, dst) in enumerate(((tokens, tok_v), (out_grad, grad_v))):
            for u in range(C):
                pltpu.make_async_remote_copy(
                    src_ref=src.at[:, pl.ds(column(g, u, 1 - core), M)],
                    dst_ref=dst.at[g, u, pl.ds(T, T)],
                    send_sem=swap_out.at[g, a],
                    recv_sem=swap_sem.at[g, a],
                    device_id=twin,
                    device_id_type=MESH,
                ).start()

    for g in groups:
        load(g)

    barrier = pltpu.get_barrier_semaphore()
    peers = [twin] + seq_peer + batch_peer
    for peer in peers:
        pl.semaphore_signal(barrier, inc=1, device_id=peer, device_id_type=MESH)
    pl.semaphore_wait(barrier, len(peers))

    for i, ref in enumerate(pre):
        pltpu.make_async_remote_copy(
            src_ref=ref, dst_ref=raw.at[i, pl.ds(T, T)], send_sem=raw_sem.at[1], recv_sem=raw_sem.at[2],
            device_id=twin, device_id_type=MESH,
        ).start()
    for g in groups:
        swap(g)

    def activate(side):
        step = 32
        def body(i, carry):
            at = pl.ds(pl.multiple_of(side * T + i * step, step), step)
            gate_val = raw[0, at, :].astype(jnp.float32)
            up_val = raw[1, at, :].astype(jnp.float32)
            grad_val = raw[2, at, :].astype(jnp.float32)
            sig = jax.nn.sigmoid(gate_val)
            act = gate_val * sig
            F = p.hidden
            hid[at, 0:F] = (grad_val * up_val * sig * (1.0 + gate_val * (1.0 - sig))).astype(jnp.bfloat16)
            hid[at, F:2 * F] = (grad_val * act).astype(jnp.bfloat16)
            hid[at, 2 * F:3 * F] = (act * up_val).astype(jnp.bfloat16)
            return carry
        lax.fori_loop(0, T // step, body, 0)

    def wait_bytes(ref, sem):
        pltpu.make_async_copy(ref, ref, sem).wait()

    wait_bytes(raw.at[:, pl.ds(0, T)], raw_sem.at[0])
    activate(0)
    wait_bytes(raw.at[:, pl.ds(T, T)], raw_sem.at[2])
    activate(1)

    def arrive(g):
        for a, dst in enumerate((tok_v, grad_v)):
            wait_bytes(dst.at[g, :, pl.ds(0, T)], load_sem.at[g, a])
            wait_bytes(dst.at[g, :, pl.ds(T, T)], swap_sem.at[g, a])

    def compute_block(g, u):
        feats, grads = tok_v[g, u], grad_v[g, u]
        for cls, (lo, hi) in enumerate(p.spans):
            pos = p.position(cls, u)
            for a, b in p.pieces(lo, hi, 2 * p.hidden):
                value = lax.dot_general(
                    feats if a < 2 * p.hidden else grads, hid[:, a:b],
                    (((0,), (0,)), ((), ())), preferred_element_type=jnp.float32,
                ).astype(jnp.bfloat16)
                for h in range(p.group):
                    m = g if p.group == 1 else g * p.group + flip(b_me % p.group, h)
                    terms[cls][m, pos, :, a - lo:b - lo] = value[h * R:(h + 1) * R]

    def compute(g):
        arrive(g)

        def body(u, carry):
            compute_block(g, u)
            return carry
        lax.fori_loop(0, C, body, 0)

    step = min(R, 32)

    def gather(cls, m, first, count, extra):
        def body(i, carry):
            blk, at = first + i // (R // step), pl.ds(pl.multiple_of((i % (R // step)) * step, step), step)
            value = terms[cls][m, blk, at, :].astype(jnp.float32)
            for ref, slot in extra:
                value = value + ref[slot, blk, at, :].astype(jnp.float32)
            terms[cls][m, blk, at, :] = value.astype(jnp.bfloat16)
            return carry
        if extra:
            lax.fori_loop(0, count * (R // step), body, 0)

    def finish(cls, extra):
        lo, hi = p.spans[cls]
        def body(i, carry):
            at = pl.ds(pl.multiple_of(i * step, step), step)
            for a, b in p.pieces(lo, hi, p.hidden):
                value = terms[cls][0, 0, at, a - lo:b - lo].astype(jnp.float32)
                for ref, slot in extra:
                    value = value + ref[slot, 0, at, a - lo:b - lo].astype(jnp.float32)
                base = (a // p.hidden) * p.hidden
                outs[a // p.hidden][at, a - base:b - base] = value
            return carry
        lax.fori_loop(0, R // step, body, 0)

    def seq_slot(cls, m):
        return 0 if p.batch_first[cls] else m

    def halves(stage):
        return 2 if C >> (stage + 1) > 1 else 1

    def seq_copy(cls, m, stage, part):
        count = C >> (stage + 1)
        size = count // halves(stage)
        first = count - size if part == 0 else 0
        slot = seq_slot(cls, m)
        return pltpu.make_async_remote_copy(
            src_ref=terms[cls].at[m, pl.ds(count + first, size)],
            dst_ref=seq_in[cls][stage].at[slot, pl.ds(first, size)],
            send_sem=seq_send.at[cls, 2 * stage + part, slot],
            recv_sem=seq_recv.at[cls, 2 * stage + part, slot],
            device_id=seq_peer[p.seq_bit(cls, stage)],
            device_id_type=MESH,
        )

    def batch_copy(cls, m):
        stage = low_bit(m)
        slot = m >> (stage + 1)
        count = C if p.batch_first[cls] else 1
        return pltpu.make_async_remote_copy(
            src_ref=terms[cls].at[m, pl.ds(0, count)],
            dst_ref=batch_in[cls][stage].at[slot],
            send_sem=batch_send.at[cls, stage, slot],
            recv_sem=batch_recv.at[cls, stage, slot],
            device_id=batch_peer[stage],
            device_id_type=MESH,
        )

    def start(copy):
        copy.start()
        sends.append(copy)

    def from_seq(cls, m, stages):
        return [(seq_in[cls][j], seq_slot(cls, m)) for j in range(stages)]

    def from_batch(cls, m):
        count = bb if m == 0 else low_bit(m)
        return [(batch_in[cls][j], m >> (j + 1)) for j in range(count)]

    def wait_batch(cls, m):
        count = bb if m == 0 else low_bit(m)
        for j in range(count):
            batch_copy(cls, m + (1 << j)).wait_recv()

    def wait_seq(cls, m, stage):
        if stage >= 0:
            seq_copy(cls, m, stage, 0).wait_recv()
        if stage >= 1:
            seq_copy(cls, m, stage - 1, 1).wait_recv()

    def seq_stage(cls, m, stage, base, parts=(0, 1)):
        wait_seq(cls, m, stage - 1)
        count = C >> (stage + 1)
        gather(cls, m, count, count, base + from_seq(cls, m, stage))
        for part in parts[:halves(stage)]:
            start(seq_copy(cls, m, stage, part))

    def batch_last(cls, m):
        wait_seq(cls, m, sb - 1)
        wait_batch(cls, m)
        extra = from_seq(cls, m, sb) + from_batch(cls, m)
        if m == 0:
            finish(cls, extra)
        else:
            gather(cls, m, 0, 1, extra)
            start(batch_copy(cls, m))

    def batch_early(cls, m):
        wait_batch(cls, m)
        if m:
            gather(cls, m, 0, C, from_batch(cls, m))
            start(batch_copy(cls, m))
        else:
            seq_stage(cls, 0, 0, from_batch(cls, 0))

    plain = [c for c in range(n_cls) if not p.batch_first[c]]
    early = [c for c in range(n_cls) if p.batch_first[c]]
    order = list(range(NB - 1, -1, -1))
    done = set()

    def need(i):
        if i < NB and order[i] // p.group not in done:
            done.add(order[i] // p.group)
            compute(order[i] // p.group)

    def first_round():
        g = groups[0]
        done.add(g)
        arrive(g)
        upper = [u for u in range(C) if any(p.position(c, u) >= C - C // 4 for c in plain)] if p.group == 1 else []
        for u in upper:
            compute_block(g, u)
        split = bool(upper) and halves(0) == 2
        if split:
            for cls in plain:
                start(seq_copy(cls, order[0], 0, 0))
        rest = [u for u in range(C) if u not in upper]
        if rest == list(range(len(rest))):
            def body(u, carry):
                compute_block(g, u)
                return carry
            lax.fori_loop(0, len(rest), body, 0)
        else:
            for u in rest:
                compute_block(g, u)
        for cls in plain:
            for part in range(1 if split else 0, halves(0)):
                start(seq_copy(cls, order[0], 0, part))
        if order[0] % 2:
            for cls in early:
                batch_early(cls, order[0])

    first_round()
    for i in range(1, NB + 1):
        before = order[i - 1]
        need(i)
        if i == 1:
            need(2)
        for stage in range(1, sb):
            for cls in plain:
                seq_stage(cls, before, stage, [])
        if i < NB:
            for cls in plain:
                seq_stage(cls, order[i], 0, [])
        if i + 1 < NB:
            need(i + 1)
        for cls in early:
            if i + 1 < NB and order[i + 1] % 2:
                batch_early(cls, order[i + 1])
            if i < NB and order[i] % 2 == 0:
                batch_early(cls, order[i])
        if i == NB:
            for stage in range(1, sb):
                for cls in early:
                    seq_stage(cls, 0, stage, from_batch(cls, 0))
        for cls in plain:
            batch_last(cls, before)
    for cls in early:
        wait_seq(cls, 0, sb - 1)
        finish(cls, from_batch(cls, 0) + from_seq(cls, 0, sb))

    for copy in sends:
        copy.wait_send()
    wait_bytes(raw.at[:, pl.ds(T, T)], raw_sem.at[1])
    for g in groups:
        for a, dst in enumerate((tok_v, grad_v)):
            wait_bytes(dst.at[g, :, pl.ds(T, T)], swap_out.at[g, a])


def on_device(n_batch, n_seq, tokens, out_grad, gate_pre, up_pre, hidden_grad):
    tok, width = tokens.shape
    hidden = gate_pre.shape[1]
    p = Plan(n_batch, n_seq, tok, width, hidden)
    C, R, bf16 = p.chips, p.rows, jnp.bfloat16
    scratch = [
        pltpu.VMEM((3, 2 * tok, hidden), bf16),
        pltpu.VMEM((2 * tok, 3 * hidden), bf16),
        pltpu.VMEM((p.n_groups, C, 2 * tok, p.block), bf16),
        pltpu.VMEM((p.n_groups, C, 2 * tok, p.block), bf16),
    ]
    sizes = [hi - lo for lo, hi in p.spans]
    scratch += [pltpu.VMEM((n_batch, C, R, size), bf16) for size in sizes]
    for cls, size in enumerate(sizes):
        slots = 1 if p.batch_first[cls] else n_batch
        scratch += [pltpu.VMEM((slots, C >> (j + 1), R, size), bf16) for j in range(p.seq_bits)]
    for cls, size in enumerate(sizes):
        blocks = C if p.batch_first[cls] else 1
        scratch += [pltpu.VMEM((n_batch >> (j + 1), blocks, R, size), bf16) for j in range(p.batch_bits)]
    n_cls = len(sizes)
    dma = pltpu.SemaphoreType.DMA
    scratch += [
        dma((3,)),
        dma((p.n_groups, 2)), dma((p.n_groups, 2)), dma((p.n_groups, 2)),
        dma((n_cls, 2 * p.seq_bits, n_batch)), dma((n_cls, 2 * p.seq_bits, n_batch)),
        dma((n_cls, p.batch_bits, n_batch // 2)), dma((n_cls, p.batch_bits, n_batch // 2)),
    ]
    out = jax.ShapeDtypeStruct((R, hidden), jnp.float32)
    return pl.pallas_call(
        functools.partial(kernel, p),
        out_shape=(out, out, out),
        in_specs=[pl.BlockSpec(memory_space=pltpu.HBM)] * 5,
        out_specs=[pl.BlockSpec(memory_space=pltpu.VMEM)] * 3,
        scratch_shapes=scratch,
        compiler_params=pltpu.CompilerParams(
            collective_id=0, has_side_effects=True, vmem_limit_bytes=67043328
        ),
    )(tokens, out_grad, gate_pre, up_pre, hidden_grad)


def solution(mesh):
    rows = P(("batch", "seq"), None)
    outs = P(("seq", "batch"), None)
    body = functools.partial(on_device, mesh.shape["batch"], mesh.shape["seq"])
    return jax.shard_map(
        body, mesh=mesh, in_specs=(rows,) * 5, out_specs=(outs,) * 3, check_vma=False
    )
```
